32 devices in a mesh: fsdp: 16 (over z, y, core), tp: 2 (over x).
Axes of the slice: x: 2, y: 2, z: 4, core: 2. Of those that a mesh axis runs over, the one named last changes fastest.
Arguments:
- tokens: bfloat16 [6144, 5632], P('fsdp', 'tp'), may hold values from -6 to 6
- gain: float32 [5632], replicated, may hold values from 0.1 to 1.9
- query_projection_weight: bfloat16 [5632, 6144], P('fsdp', 'tp'), may hold values from -0.078125 to 0.078125
- key_projection_weight: bfloat16 [5632, 1024], P('fsdp', 'tp'), may hold values from -0.078125 to 0.078125
- value_projection_weight: bfloat16 [5632, 1024], P('fsdp', 'tp'), may hold values from -0.078125 to 0.078125
- adapter_down_factors: bfloat16 [3, 16, 5632], replicated, may hold values from -0.078125 to 0.078125
- query_adapter_up: bfloat16 [16, 6144], P(None, 'tp'), may hold values from -0.078125 to 0.078125
- key_adapter_up: bfloat16 [16, 1024], P(None, 'tp'), may hold values from -0.1875 to 0.1875
- value_adapter_up: bfloat16 [16, 1024], P(None, 'tp'), may hold values from -0.1875 to 0.1875
- query_cotangent: bfloat16 [6144, 6144], P('fsdp', 'tp'), may hold values from -6 to 6
- key_cotangent: bfloat16 [6144, 1024], P('fsdp', 'tp'), may hold values from -6 to 6
- value_cotangent: bfloat16 [6144, 1024], P('fsdp', 'tp'), may hold values from -6 to 6
Outputs:
- grad_tokens: bfloat16 [6144, 5632], P('fsdp', 'tp')
- grad_down: float32 [3, 16, 5632], P(None, None, 'tp')
- grad_up_query: float32 [16, 6144], P(None, 'tp')
- grad_up_key: float32 [16, 1024], P(None, 'tp')
- grad_up_value: float32 [16, 1024], P(None, 'tp')
The draws below stay inside these ranges and needn't reach their ends.
All inputs are finite; a program needn't handle non-finite values.
Results may differ from the reference program's by a relative error of at most 0.0096.
Values may be sent and summed in bfloat16 or wider, within the bound.
No kernel may reach another device: no remote copies, remote signals or barrier semaphores. Data moves between devices by JAX's collectives and lax.ppermute only.
A program may use at most 128 MiB of HBM per device.

```python
import math
import jax
import jax.numpy as jnp
from jax import lax

MODEL_WIDTH = 5632
ADAPTER_RANK = 16
QUERY_WIDTH = 6144
KEY_VALUE_WIDTH = 1024
TOKEN_TOTAL = 6144


def steps_of(stream_key, dims, pieces, low, largest):
    factor_of = 1.0
    for dim, blocks in pieces:
        draws = jax.random.uniform(jax.random.fold_in(jax.random.fold_in(stream_key, 6), dim), (blocks,), jnp.float32, low / len(pieces), largest / len(pieces))
        factor_of = factor_of * jnp.repeat(jnp.exp(draws), dims[dim] // blocks).reshape((-1,) + (1,) * (len(dims) - 1 - dim))
    return factor_of


def scatter_about(key, extent, scale, most, split=(), kind=jnp.bfloat16):
    level = steps_of(key, extent, split, -0.22, 0.18) if split else 1.0
    drawn = jax.random.normal(key, extent, jnp.float32) * scale * level
    return jnp.minimum(jnp.maximum(drawn, -most), most).astype(kind)


def setup_inputs(seed: int = 0) -> dict:
    splits = jax.random.split(jax.random.key(seed), 13)
    return {
        "tokens": scatter_about(splits[0], (TOKEN_TOTAL, MODEL_WIDTH), 1.0, 6.0, ((0, 16), (1, 2))),
        "gain": jnp.clip(1.0 + 0.18 * jax.random.normal(splits[1], (MODEL_WIDTH,), jnp.float32), 0.1, 1.9),
        "query_projection_weight": scatter_about(splits[2], (MODEL_WIDTH, QUERY_WIDTH), MODEL_WIDTH ** -0.5, 0.078125, ((0, 16), (1, 2))),
        "key_projection_weight": scatter_about(splits[3], (MODEL_WIDTH, KEY_VALUE_WIDTH), MODEL_WIDTH ** -0.5, 0.078125, ((0, 16), (1, 2))),
        "value_projection_weight": scatter_about(splits[4], (MODEL_WIDTH, KEY_VALUE_WIDTH), MODEL_WIDTH ** -0.5, 0.078125, ((0, 16), (1, 2))),
        "adapter_down_factors": scatter_about(splits[5], (3, ADAPTER_RANK, MODEL_WIDTH), MODEL_WIDTH ** -0.5, 0.078125),
        "query_adapter_up": scatter_about(splits[6], (ADAPTER_RANK, QUERY_WIDTH), QUERY_WIDTH ** -0.5, 0.078125, ((1, 2),)),
        "key_adapter_up": scatter_about(splits[7], (ADAPTER_RANK, KEY_VALUE_WIDTH), KEY_VALUE_WIDTH ** -0.5, 0.1875, ((1, 2),)),
        "value_adapter_up": scatter_about(splits[8], (ADAPTER_RANK, KEY_VALUE_WIDTH), KEY_VALUE_WIDTH ** -0.5, 0.1875, ((1, 2),)),
        "query_cotangent": scatter_about(splits[9], (TOKEN_TOTAL, QUERY_WIDTH), 1.0, 6.0, ((0, 16), (1, 2))),
        "key_cotangent": scatter_about(splits[10], (TOKEN_TOTAL, KEY_VALUE_WIDTH), 1.0, 6.0, ((0, 16), (1, 2))),
        "value_cotangent": scatter_about(splits[11], (TOKEN_TOTAL, KEY_VALUE_WIDTH), 1.0, 6.0, ((0, 16), (1, 2))),
    }


norm_eps = 1e-05
adapter_scale = 2.0

def reference(tokens, gain, query_projection_weight, key_projection_weight, value_projection_weight, adapter_down_factors, query_adapter_up, key_adapter_up, value_adapter_up, query_cotangent, key_cotangent, value_cotangent):
    weights = (query_projection_weight, key_projection_weight, value_projection_weight)
    adapter_up_factors = (query_adapter_up, key_adapter_up, value_adapter_up)
    cotangent_list = (query_cotangent, key_cotangent, value_cotangent)
    token_width_matrix = tokens.astype(jnp.float32)
    inverse_root_mean = lax.rsqrt(lax.optimization_barrier(jnp.mean(token_width_matrix * token_width_matrix, axis=1, keepdims=True)) + norm_eps)
    unit_rows = token_width_matrix * inverse_root_mean
    scaled_input = unit_rows * gain[None, :]
    normed = scaled_input.astype(jnp.bfloat16)
    adapter_input = jnp.stack([jnp.dot(scaled_input, adapter_down_factors[slice_member].astype(jnp.float32).T, precision=lax.Precision.HIGHEST) for slice_member in range(3)])
    adapter_output = jnp.stack([jnp.dot(cotangent_list[slice_member], adapter_up_factors[slice_member].T, preferred_element_type=jnp.float32) for slice_member in range(3)])
    input_lowrank = adapter_input.astype(jnp.bfloat16)
    output_lowrank = adapter_output.astype(jnp.bfloat16)
    gradient_scale = adapter_scale / math.sqrt(TOKEN_TOTAL)
    backward_result = jnp.zeros(tokens.shape, jnp.float32)
    for slice_member in range(3):
        backward_result = backward_result + jnp.dot(cotangent_list[slice_member], weights[slice_member].T, preferred_element_type=jnp.float32)
    for slice_member in range(3):
        backward_result = backward_result + adapter_scale * jnp.dot(output_lowrank[slice_member], adapter_down_factors[slice_member], preferred_element_type=jnp.float32)
    gained = gain[None, :] * backward_result
    inner = lax.optimization_barrier(jnp.mean(gained * unit_rows, axis=1, keepdims=True))
    grad_tokens = (inverse_root_mean * (gained - unit_rows * inner)).astype(jnp.bfloat16)
    grad_down = jnp.stack([gradient_scale * jnp.dot(output_lowrank[slice_member].T, normed, preferred_element_type=jnp.float32) for slice_member in range(3)])
    grad_ups = [gradient_scale * jnp.dot(input_lowrank[slice_member].T, cotangent_list[slice_member], preferred_element_type=jnp.float32) for slice_member in range(3)]
    return (grad_tokens, grad_down, grad_ups[0], grad_ups[1], grad_ups[2])
```

```python
import functools
import math

import jax
import jax.numpy as jnp
from jax import lax
from jax.experimental import pallas as pl
from jax.experimental.pallas import tpu as pltpu
from jax.sharding import PartitionSpec as P


norm_eps = 1e-05
adapter_scale = 2.0


def transposed_product(cotangent, piece):
    return lax.dot_general(
        cotangent, piece, (((1,), (1,)), ((), ())), preferred_element_type=jnp.float32
    )


def shards(
    tokens,
    gain,
    query_projection_weight,
    key_projection_weight,
    value_projection_weight,
    adapter_down_factors,
    query_adapter_up,
    key_adapter_up,
    value_adapter_up,
    query_cotangent,
    key_cotangent,
    value_cotangent,
):
    adapter_up_factors = (query_adapter_up, key_adapter_up, value_adapter_up)
    cotangent_list = (query_cotangent, key_cotangent, value_cotangent)
    tensor_slice_index = lax.axis_index("tp")
    number_of_rows, owned_width = tokens.shape
    full_width = gain.shape[0]
    token_width_matrix = tokens.astype(jnp.float32)
    gain_own = lax.dynamic_slice_in_dim(gain, tensor_slice_index * owned_width, owned_width, 0)
    down_owned_slice = lax.dynamic_slice_in_dim(
        adapter_down_factors, tensor_slice_index * owned_width, owned_width, 2
    )
    scaled_part = token_width_matrix * gain_own[None, :]
    adapter_input_slice = jnp.einsum(
        "td,krd->ktr",
        scaled_part,
        down_owned_slice.astype(jnp.float32),
        precision=lax.Precision.HIGHEST,
    )
    adapter_output_slice = jnp.stack(
        [
            jnp.dot(
                cotangent_list[slice_member],
                adapter_up_factors[slice_member].T,
                preferred_element_type=jnp.float32,
            )
            for slice_member in range(3)
        ]
    )
    squared_total, adapter_input_unnormed, adapter_output = lax.psum(
        (
            jnp.sum(token_width_matrix * token_width_matrix, axis=1),
            adapter_input_slice,
            adapter_output_slice,
        ),
        "tp",
    )
    inverse_root_mean = lax.rsqrt(squared_total / full_width + norm_eps)[:, None]
    adapter_input = adapter_input_unnormed * inverse_root_mean[None]
    unit_rows = token_width_matrix * inverse_root_mean
    normed = (unit_rows * gain_own[None, :]).astype(jnp.bfloat16)
    input_lowrank = adapter_input.astype(jnp.bfloat16)
    output_lowrank = adapter_output.astype(jnp.bfloat16)
    gradient_scale = adapter_scale / math.sqrt(number_of_rows * lax.axis_size("fsdp"))
    down_local = gradient_scale * jnp.einsum(
        "ktr,td->krd", output_lowrank, normed, preferred_element_type=jnp.float32
    )
    up_local = tuple(
        (
            gradient_scale
            * jnp.dot(
                input_lowrank[slice_member].T,
                cotangent_list[slice_member],
                preferred_element_type=jnp.float32,
            )
            for slice_member in range(3)
        )
    )
    grad_down, grad_up_query, grad_up_key, grad_up_value = lax.psum(
        (down_local, up_local[0], up_local[1], up_local[2]), "fsdp"
    )
    empty = jnp.zeros((number_of_rows, full_width), jnp.float32)

    def adder(cotangent, total, piece):
        return total + transposed_product(cotangent, piece)

    partial_back = adder(
        query_cotangent, empty, lax.all_gather(query_projection_weight, "fsdp", axis=0, tiled=True)
    )
    partial_back = adder(
        key_cotangent,
        partial_back,
        lax.all_gather(key_projection_weight, "fsdp", axis=0, tiled=True),
    )
    partial_back = adder(
        value_cotangent,
        partial_back,
        lax.all_gather(value_projection_weight, "fsdp", axis=0, tiled=True),
    )
    backward_result = lax.psum_scatter(partial_back, "tp", scatter_dimension=1, tiled=True)
    backward_result = backward_result + adapter_scale * jnp.einsum(
        "ktr,krd->td", output_lowrank, down_owned_slice, preferred_element_type=jnp.float32
    )
    gained = gain_own[None, :] * backward_result
    inner = lax.psum(jnp.sum(gained * unit_rows, axis=1), "tp") / full_width
    grad_tokens = (inverse_root_mean * (gained - unit_rows * inner[:, None])).astype(jnp.bfloat16)
    return (grad_tokens, grad_down, grad_up_query, grad_up_key, grad_up_value)


def line_ring(length):
    evens = list(range(0, length, 2))
    odds = list(range(1, length, 2))
    return evens + odds[::-1]


def chunk_bounds(rows):
    first = max(16, rows // 32 * 16)
    return ((0, first), (first, rows))


def group_size_of(members):
    size = 1
    while size * size < members and members % (size * 2) == 0:
        size *= 2
    return size


def exchange(value):
    return lax.ppermute(value, "tp", [(0, 1), (1, 0)])


def from_partner(value, members, offset):
    return lax.ppermute(value, "fsdp", [(m, m ^ offset) for m in range(members)])


def halves(value, dim, bit):
    size = value.shape[dim] // 2
    mine = lax.dynamic_slice_in_dim(value, bit * size, size, dim)
    other = lax.dynamic_slice_in_dim(value, (1 - bit) * size, size, dim)
    return mine, other


def member_sum(values, member, members, inner_size):
    values = list(values)
    levels = []
    offset, dim = 1, 1
    while offset < inner_size:
        bit = (member // offset) % 2
        for i, value in enumerate(values):
            mine, other = halves(value, dim, bit)
            other = from_partner(other, members, offset)
            values[i] = mine + other
        levels.append((offset, dim, bit))
        offset, dim = offset * 2, 0
    while offset < members:
        for i, value in enumerate(values):
            other = from_partner(value, members, offset)
            values[i] = value + other
        offset *= 2
    for offset, dim, bit in levels[::-1]:
        for i, mine in enumerate(values):
            other = from_partner(mine, members, offset)
            low = jnp.where(bit == 0, mine, other)
            high = jnp.where(bit == 0, other, mine)
            values[i] = jnp.concatenate([low, high], axis=dim)
    return tuple(values)


def assemble_kernel(count, starts, *refs):
    parts, (low, down, gain, tokens, gained, inner, back) = refs[:count], refs[count:]
    for i, part in enumerate(parts):
        back[pl.ds(pl.multiple_of(starts[i], 16), part.shape[0]), :] = part[...]
    lanes = 128
    total = jnp.zeros((tokens.shape[0], lanes), jnp.float32)

    def tile(k, total):
        columns = pl.ds(pl.multiple_of(k * lanes, lanes), lanes)
        value = back[columns, :].astype(jnp.float32).T
        value = value + jnp.dot(low[...], down[:, columns], preferred_element_type=jnp.float32)
        value = value * gain[:, columns]
        gained[:, columns] = value
        return total + value * tokens[:, columns].astype(jnp.float32)

    total = lax.fori_loop(0, tokens.shape[1] // lanes, tile, total)
    inner[...] = jnp.broadcast_to(jnp.sum(total, axis=1, keepdims=True), inner.shape)


def assemble(starts, parts, low, down, gain, tokens):
    rows, width = tokens.shape
    vmem = pl.BlockSpec(memory_space=pltpu.VMEM)
    return pl.pallas_call(
        functools.partial(assemble_kernel, len(parts)),
        out_shape=(
            jax.ShapeDtypeStruct((rows, width), jnp.float32),
            jax.ShapeDtypeStruct((rows, 128), jnp.float32),
        ),
        in_specs=[pl.BlockSpec(memory_space=pltpu.SMEM)] + [vmem] * (len(parts) + 4),
        out_specs=(vmem, vmem),
        scratch_shapes=[pltpu.VMEM((width, rows), jnp.bfloat16)],
        cost_estimate=pl.CostEstimate(
            flops=2 * rows * width * low.shape[1],
            bytes_accessed=rows * width * 10,
            transcendentals=0,
        ),
    )(starts, *parts, low, down, gain, tokens)


def ring_shards(
    tokens,
    gain,
    query_projection_weight,
    key_projection_weight,
    value_projection_weight,
    adapter_down_factors,
    query_adapter_up,
    key_adapter_up,
    value_adapter_up,
    query_cotangent,
    key_cotangent,
    value_cotangent,
):
    adapter_up_factors = (query_adapter_up, key_adapter_up, value_adapter_up)
    cotangent_list = (query_cotangent, key_cotangent, value_cotangent)
    tensor_slice_index = lax.axis_index("tp")
    member = lax.axis_index("fsdp")
    members = lax.axis_size("fsdp")
    inner_size = group_size_of(members)
    outer_size = members // inner_size
    half = outer_size // 2
    order = line_ring(outer_size)
    place, seat = member // inner_size, member % inner_size
    number_of_rows, owned_width = tokens.shape
    full_width = gain.shape[0]
    block_rows = query_projection_weight.shape[0]
    bounds = chunk_bounds(block_rows)
    chunks = len(bounds)

    own_rows = [
        jnp.concatenate(
            [
                w[low:high]
                for w in (query_projection_weight, key_projection_weight, value_projection_weight)
            ],
            axis=1,
        )
        for low, high in bounds
    ]
    ring_pairs = [
        (order[i] * inner_size + s, order[(i + 1) % outer_size] * inner_size + s)
        for i in range(outer_size)
        for s in range(inner_size)
    ]
    held = [own_rows]
    for _ in range(outer_size - 1):
        passed = []
        for piece in held[-1]:
            passed.append(lax.ppermute(piece, "fsdp", ring_pairs))
        held.append(passed)

    cot_blocks = jnp.concatenate(cotangent_list, axis=1)
    offset = inner_size // 2
    offsets = [0]
    while offset:
        other_rows = from_partner(cot_blocks, members, offset)
        cot_blocks = jnp.concatenate([cot_blocks, other_rows], axis=0)
        offsets = offsets + [o ^ offset for o in offsets]
        offset //= 2

    token_width_matrix = tokens.astype(jnp.float32)
    gain_own = lax.dynamic_slice_in_dim(gain, tensor_slice_index * owned_width, owned_width, 0)
    down_owned_slice = lax.dynamic_slice_in_dim(
        adapter_down_factors, tensor_slice_index * owned_width, owned_width, 2
    )
    scaled_part = token_width_matrix * gain_own[None, :]
    adapter_input_slice = jnp.einsum(
        "td,krd->ktr",
        scaled_part,
        down_owned_slice.astype(jnp.float32),
        precision=lax.Precision.HIGHEST,
    )
    adapter_output_slice = jnp.stack(
        [
            jnp.dot(
                cotangent_list[slice_member],
                adapter_up_factors[slice_member].T,
                preferred_element_type=jnp.float32,
            )
            for slice_member in range(3)
        ]
    )
    squared_part = jnp.sum(token_width_matrix * token_width_matrix, axis=1)
    packed = jnp.concatenate(
        [adapter_input_slice, adapter_output_slice], axis=0
    )
    packed = packed + exchange(packed)
    squared_total = squared_part + exchange(squared_part)
    adapter_input_unnormed, adapter_output = packed[:3], packed[3:]
    inverse_root_mean = lax.rsqrt(squared_total / full_width + norm_eps)[:, None]
    adapter_input = adapter_input_unnormed * inverse_root_mean[None]
    unit_rows = token_width_matrix * inverse_root_mean
    normed = (unit_rows * gain_own[None, :]).astype(jnp.bfloat16)
    input_lowrank = adapter_input.astype(jnp.bfloat16)
    output_lowrank = adapter_output.astype(jnp.bfloat16)
    gradient_scale = adapter_scale / math.sqrt(number_of_rows * members)
    down_local = gradient_scale * jnp.einsum(
        "ktr,td->krd", output_lowrank, normed, preferred_element_type=jnp.float32
    )
    up_local = tuple(
        gradient_scale
        * jnp.dot(
            input_lowrank[slice_member].T,
            cotangent_list[slice_member],
            preferred_element_type=jnp.float32,
        )
        for slice_member in range(3)
    )
    rank = adapter_down_factors.shape[1]
    grads = member_sum(
        (down_local.reshape(3 * rank, owned_width), jnp.concatenate(up_local, axis=1)),
        member,
        members,
        inner_size,
    )

    position = jnp.array([order.index(z) for z in range(outer_size)], jnp.int32)[place]
    order_table = jnp.array(order, jnp.int32)
    parts, starts = [], []
    partial = {}

    def send_on(step, c):
        first = step - half
        early_place = order_table[(position - first) % outer_size]
        late_place = order_table[(position - step) % outer_size]
        early_owned = early_place // half == tensor_slice_index
        owned_place = jnp.where(early_owned, early_place, late_place) % half
        early, late = partial[first][c], partial[step][c]
        kept = jnp.where(early_owned, early, late)
        sent = jnp.where(early_owned, late, early)
        swapped = exchange(sent)
        summed = (kept.astype(jnp.float32) + swapped.astype(jnp.float32)).astype(jnp.bfloat16)
        for r, o in enumerate(offsets):
            part = summed[:, r * number_of_rows : (r + 1) * number_of_rows]
            if o:
                part = from_partner(part, members, o)
            start = (owned_place * inner_size + (seat ^ o)) * block_rows + bounds[c][0]
            parts.append(part)
            starts.append(start)

    for step in range(outer_size):
        partial[step] = []
        for c, piece in enumerate(held[step]):
            if step == outer_size - 1 and c == chunks - 1:
                early_parts = (half - 1) * chunks * inner_size
                piece, grads, parts[:early_parts], early_low = lax.optimization_barrier(
                    (piece, grads, parts[:early_parts], (output_lowrank, inverse_root_mean))
                )
                output_lowrank, inverse_root_mean = early_low
            product = lax.dot_general(
                piece, cot_blocks, (((1,), (1,)), ((), ())), preferred_element_type=jnp.float32
            ).astype(jnp.bfloat16)
            partial[step].append(lax.optimization_barrier(product))
            if step >= half:
                send_on(step, c)

    low = (adapter_scale * output_lowrank).transpose(1, 0, 2).reshape(number_of_rows, 3 * rank)
    gained, inner_part = assemble(
        jnp.stack(starts).astype(jnp.int32),
        parts,
        low,
        down_owned_slice.reshape(3 * rank, owned_width),
        gain_own[None, :],
        tokens,
    )
    inner_part = inner_part[:, 0] * inverse_root_mean[:, 0]
    inner = (inner_part + exchange(inner_part)) / full_width
    unit_rows = tokens.astype(jnp.float32) * inverse_root_mean
    grad_tokens = (inverse_root_mean * (gained - unit_rows * inner[:, None])).astype(jnp.bfloat16)
    query_width = query_cotangent.shape[1]
    key_end = query_width + key_cotangent.shape[1]
    grad_down, grad_up = grads
    return (
        grad_tokens,
        grad_down.reshape(3, rank, owned_width),
        grad_up[:, :query_width],
        grad_up[:, query_width:key_end],
        grad_up[:, key_end:],
    )


def solution(mesh):
    in_specs = (
        P("fsdp", "tp"),
        P(),
        P("fsdp", "tp"),
        P("fsdp", "tp"),
        P("fsdp", "tp"),
        P(),
        P(None, "tp"),
        P(None, "tp"),
        P(None, "tp"),
        P("fsdp", "tp"),
        P("fsdp", "tp"),
        P("fsdp", "tp"),
    )
    out_specs = (P("fsdp", "tp"), P(None, None, "tp"), P(None, "tp"), P(None, "tp"), P(None, "tp"))
    members, slices = mesh.shape["fsdp"], mesh.shape["tp"]
    outer_size = members // group_size_of(members)
    ring = slices == 2 and outer_size % 2 == 0
    if ring:
        return jax.shard_map(
            ring_shards, mesh=mesh, in_specs=in_specs, out_specs=out_specs, check_vma=False
        )
    return jax.shard_map(shards, mesh=mesh, in_specs=in_specs, out_specs=out_specs, check_vma=False)
```
